256 devices in a mesh: row: 8 (over z), col: 32 (over y, x, core).
Axes of the slice: x: 4, y: 4, z: 8, core: 2. Of those that a mesh axis runs over, the one named last changes fastest.
Arguments:
- factor: bfloat16 [131072, 5, 1024], P('col', None, 'row'), may hold values from -0.0625 to 0.0625
- diag_inverse: bfloat16 [5, 1024, 1024], P(None, 'row'), may hold values from -1 to 2
- right_side: float32 [16, 128, 1024], P(None, 'col', 'row'), may hold values from -6 to 6
- tile_order: int32 [128], replicated, may hold values from 0 to 127, each once
- live_segments: int32 [16], replicated, may hold values from 2 to 5
Outputs:
- result: float32 [16, 128, 1024], P(None, 'col', 'row')
The draws below stay inside these ranges and needn't reach their ends.
Inputs may be any that keep to these rules, and one draw needn't show every extreme that they name: `tile_order`: each of 0 to 127 appears once.
All inputs are finite; a program needn't handle non-finite values.
Results may differ from the reference program's by a relative error of at most 0.0019.
Values may be sent and summed in bfloat16 or wider, within the bound.
A program may use at most 64 MiB of HBM per device.

```python
import math
import jax
import jax.numpy as jnp
from jax import lax

TB = 1024
NRHS = 16
SECTIONS = 5
K = 128
N = 131072


def draw_diag_inverse(key, part):
    identity = jnp.broadcast_to(jnp.eye(TB, dtype=jnp.float32), (SECTIONS, TB, TB))
    noise = jax.random.normal(key, (SECTIONS, TB, TB), jnp.float32) * (0.4 / math.sqrt(TB))
    return (identity + noise).astype(jnp.bfloat16)


def place_ends(values, stream_key, low, top_value):
    shape = values.shape
    place = [jax.random.randint(jax.random.fold_in(stream_key, axis), (), 0, shape[axis]) for axis in range(len(shape))]
    values = values.at[tuple(place)].set(low)
    longest = shape.index(max(shape))
    place[longest] = (place[longest] + 1) % shape[longest]
    return values.at[tuple(place)].set(top_value)


def level_of(own_key, shape, cuts, least, high):
    gain = 1.0
    for position, blocks in cuts:
        heights = jax.random.uniform(jax.random.fold_in(jax.random.fold_in(own_key, 6), position), (blocks,), jnp.float32, least / len(cuts), high / len(cuts))
        gain = gain * jnp.repeat(jnp.exp(heights), shape[position] // blocks).reshape((-1,) + (1,) * (len(shape) - 1 - position))
    return gain


def scatter_about(rng, extent, scale, limit, cuts=(), kind=jnp.bfloat16):
    loudness = level_of(rng, extent, cuts, -0.22, 0.18) if cuts else 1.0
    entries = jax.random.normal(rng, extent, jnp.float32) * scale * loudness
    return jnp.minimum(jnp.maximum(entries, -limit), limit).astype(kind)


def setup_inputs(seed: int = 0) -> dict:
    key_of = jax.random.split(jax.random.key(seed), 6)
    factor = scatter_about(key_of[0], (N, SECTIONS, TB), (2 * SECTIONS * TB) ** -0.5, 0.0625, ((0, 32), (2, 8)))
    diag_inverse = draw_diag_inverse(jax.random.fold_in(key_of[5], 71), 0)
    right_side = scatter_about(key_of[2], (NRHS, K, TB), 1.0, 6.0, ((1, 32), (2, 8)), jnp.float32)
    tile_order = jax.random.permutation(key_of[3], K).astype(jnp.int32)
    live_segments = place_ends(jax.random.randint(key_of[4], (NRHS,), SECTIONS // 2, SECTIONS + 1), jax.random.fold_in(key_of[4], 1), SECTIONS // 2, SECTIONS).astype(jnp.int32)
    return dict(factor=factor, diag_inverse=diag_inverse, right_side=right_side, tile_order=tile_order, live_segments=live_segments)


def reference(factor, diag_inverse, right_side, tile_order, live_segments):
    segment_limit = live_segments.astype(jnp.int32)
    partial_value = jnp.zeros((NRHS, K * TB), jnp.float32)
    result = jnp.zeros((NRHS, K, TB), jnp.float32)
    for section in range(SECTIONS):
        slot_id = tile_order[section].astype(jnp.int32)
        offset = (slot_id * TB).astype(jnp.int32)
        rhs_tile = lax.dynamic_index_in_dim(right_side, slot_id, 1, keepdims=False)
        remaining = rhs_tile - lax.dynamic_slice_in_dim(partial_value, offset, TB, 1)
        inverse = diag_inverse[section].astype(jnp.float32)
        solved = lax.dot_general(remaining, inverse, (((1,), (1,)), ((), ())),
                                 precision=lax.Precision.HIGHEST, preferred_element_type=jnp.float32)
        is_live = (section < segment_limit)[:, None]
        sent_block = jnp.where(is_live, solved, jnp.zeros_like(solved)).astype(jnp.bfloat16)
        partial_value = partial_value + lax.dot_general(sent_block, factor[:, section, :], (((1,), (1,)), ((), ())),
                                            preferred_element_type=jnp.float32)
        stored = jnp.where(is_live, solved, remaining)
        result = lax.dynamic_update_slice_in_dim(result, stored[:, None, :], slot_id, 1)
    slot_ids = jnp.arange(K, dtype=jnp.int32)
    visited = jnp.any(slot_ids[:, None] == tile_order[:SECTIONS][None, :], axis=1)
    trailing = right_side - partial_value.reshape(NRHS, K, TB)
    return jnp.where(visited[None, :, None], result, trailing)
```

```python
import functools
import itertools

import jax
import jax.numpy as jnp
from jax import lax
from jax.experimental import pallas as pl
from jax.experimental.pallas import tpu as pltpu
from jax.sharding import Mesh
from jax.sharding import PartitionSpec as P

MESH = pl.DeviceIdType.MESH
COL = ("y", "x", "core")
LANES = 128


def first_of(t):
    return t * (t - 1) // 2


def kernel(
    sizes,
    sections,
    order,
    live,
    f_hbm,
    d_hbm,
    rhs,
    out,
    fac,
    inv,
    low,
    core_out,
    core_in,
    plane_out,
    plane_in,
    chunk,
    b_out,
    b_in,
    z_out,
    z_in,
    x_all,
    total,
    f_out,
    f_in,
    local_sem,
    send_sem,
    recv_sem,
):
    nz, ny, nx = sizes
    chips = ny * nx
    tile = nz * LANES
    half = tile // 2
    rows_dev = rhs.shape[1]
    z = lax.axis_index("row")
    y = lax.axis_index("y")
    x = lax.axis_index("x")
    core = lax.axis_index("core")
    chip = y * nx + x
    col = chip * 2 + core

    phase_of = {}

    def phase(*key):
        return phase_of.setdefault(key, len(phase_of))

    pending = []

    def send(key, src, dst, device):
        number = phase(*key)
        pltpu.make_async_remote_copy(
            src_ref=src,
            dst_ref=dst,
            send_sem=send_sem.at[number],
            recv_sem=recv_sem.at[number],
            device_id=device,
            device_id_type=MESH,
        ).start()

    def arrived(key, like):
        pltpu.make_async_copy(like, like, recv_sem.at[phase(*key)]).wait()

    steps = sorted(
        [o for o in itertools.product(range(ny), range(nx)) if any(o)],
        key=lambda o: -(min(o[0], ny - o[0]) + min(o[1], nx - o[1])),
    )

    def chip_at(step):
        return lax.rem(y + step[0], ny), lax.rem(x + step[1], nx)

    def z_at(step):
        return lax.rem(z + step, nz)

    z_steps = sorted(range(1, nz), key=lambda o: -min(o, nz - o))

    fac_copies = []
    for u in range(sections):
        copy = pltpu.make_async_copy(f_hbm.at[u], fac.at[u], local_sem.at[u])
        copy.start()
        fac_copies.append(copy)
    inv_copy = pltpu.make_async_copy(d_hbm, inv, local_sem.at[sections])
    inv_copy.start()

    barrier = pltpu.get_barrier_semaphore()
    count = 0
    for step in steps:
        py, px = chip_at(step)
        for other in range(2):
            pl.semaphore_signal(
                barrier,
                inc=1,
                device_id={"y": py, "x": px, "core": (core + other) % 2},
                device_id_type=MESH,
            )
            count += 1
    pl.semaphore_signal(barrier, inc=1, device_id={"core": 1 - core}, device_id_type=MESH)
    count += 1
    for step in z_steps:
        pl.semaphore_signal(barrier, inc=1, device_id={"row": z_at(step)}, device_id_type=MESH)
        count += 1

    slots = [jnp.full((chips, LANES), order[t], jnp.int32) for t in range(sections)]
    own_slot = [[slots[t] == col * rows_dev + l for l in range(rows_dev)] for t in range(sections)]

    b_out[...] = jnp.zeros_like(b_out)
    for t in range(sections):
        value = jnp.zeros((chips, LANES), jnp.float32)
        for l in range(rows_dev):
            value = jnp.where(own_slot[t][l], rhs[:, l, :], value)
        b_out[:, t, :] = value

    masks = [
        [
            jnp.where(own_slot[t][l], 1.0, 0.0).astype(jnp.bfloat16)[None]
            for l in range(rows_dev)
        ]
        for t in range(sections)
    ]

    def own_half(t, u, part):
        value = None
        for l in range(rows_dev):
            start = pl.multiple_of(l * tile + part * half, half)
            rows = fac[u, pl.ds(start, half), :].reshape(half // chips, chips, LANES)
            rows = rows * masks[t][l]
            value = rows if value is None else value + rows
        return value.reshape(chips, half // chips, LANES)

    for u in range(sections):
        fac_copies[u].wait()
    for t in range(1, sections):
        for u in range(t):
            core_out[first_of(t) + u] = own_half(t, u, 1 - core)
            plane_out[first_of(t) + u] = own_half(t, u, core)

    pl.semaphore_wait(barrier, count)

    for step in steps:
        py, px = chip_at(step)
        for other in range(2):
            send(
                ("b",),
                b_out.at[py * nx + px],
                b_in.at[col],
                {"y": py, "x": px, "core": (core + other) % 2},
            )
    send(("b",), b_out.at[chip], b_in.at[col], {"core": 1 - core})
    b_in[col] = b_out[chip]

    def tiles_of(t):
        return pl.ds(first_of(t), t)

    for t in range(1, sections):
        send(("core", t), core_out.at[tiles_of(t)], core_in.at[tiles_of(t)], {"core": 1 - core})

    def scatter(t):
        arrived(("core", t), core_in.at[tiles_of(t)])
        for u in range(t):
            q = first_of(t) + u
            plane_out[q] = plane_out[q] + core_in[q]
            plane_in[chip, q] = plane_out[q, chip]
        for step in steps:
            py, px = chip_at(step)
            send(
                ("scatter", t),
                plane_out.at[tiles_of(t), py * nx + px],
                plane_in.at[chip, tiles_of(t)],
                {"y": py, "x": px},
            )

    def gather(t):
        arrived(("scatter", t), plane_in.at[pl.ds(0, chips - 1), tiles_of(t)])
        for u in range(t):
            q = first_of(t) + u
            value = plane_in[0, q]
            for j in range(1, chips):
                value = value + plane_in[j, q]
            chunk[q] = value
            low[q, core, chip] = value
        for step in steps:
            py, px = chip_at(step)
            send(
                ("gather", t),
                chunk.at[tiles_of(t)],
                low.at[tiles_of(t), core, chip],
                {"y": py, "x": px},
            )

    def swap(t):
        arrived(("gather", t), low.at[tiles_of(t), 0, pl.ds(0, chips - 1)])
        send(
            ("swap", t),
            low.at[tiles_of(t), core],
            low.at[tiles_of(t), core],
            {"core": 1 - core},
        )

    def swapped(t):
        arrived(("swap", t), low.at[tiles_of(t), 0])

    block_row = lax.broadcasted_iota(jnp.int32, (nz, LANES), 0)
    held = [jnp.zeros((nz, LANES), jnp.float32) for _ in range(sections)]
    sent = [None] * sections

    def product(t, u):
        weights = low[first_of(t) + u].reshape(tile, LANES)
        full = lax.dot_general(
            sent[u], weights, (((1,), (1,)), ((), ())), preferred_element_type=jnp.float32
        )
        value = jnp.zeros((nz, LANES), jnp.float32)
        for k in range(nz):
            value = jnp.where(block_row == k, full[0:nz, k * LANES : (k + 1) * LANES], value)
        return value

    def ask(t, b_all):
        value = jnp.where(block_row == z, b_all[t : t + 1, :], 0.0) - held[t]
        z_out[t] = value
        z_in[t, z] = value
        for step in z_steps:
            send(("z", t), z_out.at[t], z_in.at[t, z], {"row": z_at(step)})

    def solve(t):
        arrived(("z", t), z_in.at[t, pl.ds(0, nz - 1)])
        remaining = z_in[t, 0]
        for k in range(1, nz):
            remaining = remaining + z_in[t, k]
        high = remaining.astype(jnp.bfloat16).astype(jnp.float32)
        rest = remaining - high
        mid = rest.astype(jnp.bfloat16).astype(jnp.float32)
        pieces = jnp.concatenate([high, mid, rest - mid, jnp.zeros_like(high)], axis=0)
        piece_row = lax.broadcasted_iota(jnp.int32, (4 * nz, LANES), 0) % nz
        spread = jnp.concatenate(
            [jnp.where(piece_row == k, pieces, 0.0) for k in range(nz)], axis=1
        ).astype(jnp.bfloat16)
        parts = lax.dot_general(
            spread, inv[t], (((1,), (1,)), ((), ())), preferred_element_type=jnp.float32
        )
        solved = jnp.sum(parts, axis=0, keepdims=True)
        x_all[t, chip] = solved
        for step in steps:
            py, px = chip_at(step)
            send(("x", t), x_all.at[t, chip], x_all.at[t, chip], {"y": py, "x": px})
        kept = jnp.where(t < my_live, jnp.broadcast_to(solved, (chips, LANES)), 0.0)
        sent[t] = kept.astype(jnp.bfloat16)

    rhs_row = lax.broadcasted_iota(jnp.int32, (chips, LANES), 0)
    live_rows = jnp.zeros((chips, LANES), jnp.int32)
    for j in range(chips):
        live_rows = jnp.where(rhs_row == j, live[j], live_rows)
    my_live = jnp.full((chips, LANES), live[chip], jnp.int32)
    solved_all = [None] * sections

    def update(u):
        arrived(("x", u), x_all.at[u, pl.ds(0, chips - 1)])
        rows = jnp.concatenate([x_all[u, j] for j in range(chips)], axis=0)
        solved_all[u] = rows
        block = jnp.where(u < live_rows, rows, 0.0).astype(jnp.bfloat16)
        for l in range(rows_dev):
            part = lax.dot_general(
                block,
                fac[u, l * tile : (l + 1) * tile, :],
                (((1,), (1,)), ((), ())),
                preferred_element_type=jnp.float32,
            )
            total[l] = part if u == 0 else total[l] + part

    scatter(1)
    scatter(2)
    arrived(("b",), b_in.at[pl.ds(0, 2 * chips - 1)])
    b_all = b_in[0]
    for j in range(1, 2 * chips):
        b_all = b_all + b_in[j]
    ask(0, b_all)
    gather(1)
    scatter(3)
    gather(2)
    scatter(4)
    inv_copy.wait()
    solve(0)
    swap(1)
    swapped(1)
    held[1] = held[1] + product(1, 0)
    ask(1, b_all)
    swap(2)
    gather(3)
    swapped(2)
    held[2] = held[2] + product(2, 0)
    solve(1)
    held[2] = held[2] + product(2, 1)
    ask(2, b_all)
    swap(3)
    gather(4)
    update(0)
    swapped(3)
    held[3] = held[3] + product(3, 0) + product(3, 1)
    solve(2)
    held[3] = held[3] + product(3, 2)
    ask(3, b_all)
    update(1)
    swap(4)
    swapped(4)
    held[4] = held[4] + product(4, 0) + product(4, 1) + product(4, 2)
    solve(3)
    held[4] = held[4] + product(4, 3)
    ask(4, b_all)
    update(2)
    update(3)
    solve(4)
    update(4)

    for k in range(nz):
        f_out[k] = total[:, :, k * LANES : (k + 1) * LANES].astype(jnp.bfloat16)
    for step in z_steps:
        to = z_at(step)
        send(("final",), f_out.at[to], f_in.at[z], {"row": to})
    f_in[z] = f_out[z]
    arrived(("final",), f_in.at[pl.ds(0, nz - 1)])
    for l in range(rows_dev):
        value = rhs[:, l, :]
        taken = f_in[0, l].astype(jnp.float32)
        for k in range(1, nz):
            taken = taken + f_in[k, l].astype(jnp.float32)
        value = value - taken
        for u in range(sections):
            here = (u < live_rows) & own_slot[u][l]
            value = jnp.where(here, solved_all[u], value)
        out[:, l, :] = value

    def left(key, like):
        pltpu.make_async_copy(like, like, send_sem.at[phase(*key)]).wait()

    left(("b",), b_in.at[pl.ds(0, 2 * chips - 1)])
    for t in range(1, sections):
        left(("core", t), core_out.at[tiles_of(t)])
        left(("scatter", t), plane_in.at[pl.ds(0, chips - 1), tiles_of(t)])
        left(("gather", t), plane_in.at[pl.ds(0, chips - 1), tiles_of(t)])
        left(("swap", t), low.at[tiles_of(t), 0])
    for t in range(sections):
        left(("z", t), z_in.at[t, pl.ds(0, nz - 1)])
        left(("x", t), x_all.at[t, pl.ds(0, chips - 1)])
    left(("final",), f_in.at[pl.ds(0, nz - 1)])


def per_device(sizes, factor, diag_inverse, right_side, tile_order, live_segments):
    nz, ny, nx = sizes
    sections, _, tile = diag_inverse.shape
    rhs_count, rows_dev, width = right_side.shape
    chips = ny * nx
    tiles = first_of(sections)
    part = tile // (2 * chips)
    phases = 2 + 4 * (sections - 1) + 2 * sections
    bf16, f32 = jnp.bfloat16, jnp.float32
    vmem = pltpu.VMEM
    return pl.pallas_call(
        functools.partial(kernel, sizes, sections),
        out_shape=jax.ShapeDtypeStruct(right_side.shape, f32),
        in_specs=[
            pl.BlockSpec(memory_space=pltpu.SMEM),
            pl.BlockSpec(memory_space=pltpu.SMEM),
            pl.BlockSpec(memory_space=pl.ANY),
            pl.BlockSpec(memory_space=pl.ANY),
            pl.BlockSpec(memory_space=vmem),
        ],
        out_specs=pl.BlockSpec(memory_space=vmem),
        scratch_shapes=[
            vmem((sections, rows_dev * tile, width), bf16),
            vmem((sections, width, tile), bf16),
            vmem((tiles, 2, chips, part, width), bf16),
            vmem((tiles, chips, part, width), bf16),
            vmem((tiles, chips, part, width), bf16),
            vmem((tiles, chips, part, width), bf16),
            vmem((chips, tiles, part, width), bf16),
            vmem((tiles, part, width), bf16),
            vmem((rhs_count, 8, width), f32),
            vmem((2 * chips, 8, width), f32),
            vmem((sections, nz, width), f32),
            vmem((sections, nz, nz, width), f32),
            vmem((sections, chips, 1, width), f32),
            vmem((rows_dev, rhs_count, tile), f32),
            vmem((nz, rows_dev, rhs_count, width), bf16),
            vmem((nz, rows_dev, rhs_count, width), bf16),
            pltpu.SemaphoreType.DMA((sections + 1,)),
            pltpu.SemaphoreType.DMA((phases,)),
            pltpu.SemaphoreType.DMA((phases,)),
        ],
        compiler_params=pltpu.CompilerParams(collective_id=0, has_side_effects=True),
    )(tile_order, live_segments, jnp.transpose(factor, (1, 0, 2)), diag_inverse, right_side)


def solution(mesh):
    sizes = (mesh.shape["row"], 4, 4)
    finer = Mesh(mesh.devices.reshape(mesh.shape["row"], 4, 4, 2), ("row", *COL))
    return jax.shard_map(
        functools.partial(per_device, sizes),
        mesh=finer,
        in_specs=(P(COL, None, "row"), P(None, "row", None), P(None, COL, "row"), P(), P()),
        out_specs=P(None, COL, "row"),
        check_vma=False,
    )
```

```python
import functools
import itertools

import jax
import jax.numpy as jnp
from jax import lax
from jax.experimental import pallas as pl
from jax.experimental.pallas import tpu as pltpu
from jax.sharding import Mesh
from jax.sharding import PartitionSpec as P

MESH = pl.DeviceIdType.MESH
COL = ("y", "x", "core")
LANES = 128


NEAR = 2


def moved(t):
    return range(max(0, t - NEAR), t)


def first_of(t):
    return sum(len(moved(s)) for s in range(1, t))


def place_of(t, u):
    return first_of(t) + u - moved(t)[0]


def kernel(
    sizes,
    sections,
    order,
    live,
    f_hbm,
    d_hbm,
    rhs,
    out,
    fac,
    inv,
    low,
    core_out,
    core_in,
    plane_out,
    plane_in,
    chunk,
    b_out,
    b_in,
    z_out,
    z_in,
    x_all,
    total,
    back_out,
    back_in,
    f_out,
    f_in,
    local_sem,
    send_sem,
    recv_sem,
):
    nz, ny, nx = sizes
    chips = ny * nx
    tile = nz * LANES
    half = tile // 2
    rows_dev = rhs.shape[1]
    z = lax.axis_index("row")
    y = lax.axis_index("y")
    x = lax.axis_index("x")
    core = lax.axis_index("core")
    chip = y * nx + x
    col = chip * 2 + core

    phase_of = {}

    def phase(*key):
        return phase_of.setdefault(key, len(phase_of))

    pending = []

    def send(key, src, dst, device):
        number = phase(*key)
        pltpu.make_async_remote_copy(
            src_ref=src,
            dst_ref=dst,
            send_sem=send_sem.at[number],
            recv_sem=recv_sem.at[number],
            device_id=device,
            device_id_type=MESH,
        ).start()

    def arrived(key, like):
        pltpu.make_async_copy(like, like, recv_sem.at[phase(*key)]).wait()

    steps = sorted(
        [o for o in itertools.product(range(ny), range(nx)) if any(o)],
        key=lambda o: -(min(o[0], ny - o[0]) + min(o[1], nx - o[1])),
    )

    def chip_at(step):
        return lax.rem(y + step[0], ny), lax.rem(x + step[1], nx)

    def z_at(step):
        return lax.rem(z + step, nz)

    z_steps = sorted(range(1, nz), key=lambda o: -min(o, nz - o))

    barrier = pltpu.get_barrier_semaphore()
    count = 0
    for step in steps:
        py, px = chip_at(step)
        for other in range(2):
            pl.semaphore_signal(
                barrier,
                inc=1,
                device_id={"y": py, "x": px, "core": (core + other) % 2},
                device_id_type=MESH,
            )
            count += 1
    for step in z_steps:
        pl.semaphore_signal(barrier, inc=1, device_id={"row": z_at(step)}, device_id_type=MESH)
        count += 1
    pl.semaphore_signal(barrier, inc=1, device_id={"core": 1 - core}, device_id_type=MESH)
    count += 1

    fac_copies = []
    for u in range(sections):
        copy = pltpu.make_async_copy(f_hbm.at[u], fac.at[u], local_sem.at[u])
        copy.start()
        fac_copies.append(copy)
    inv_copy = pltpu.make_async_copy(d_hbm, inv, local_sem.at[sections])
    inv_copy.start()

    slots = [jnp.full((chips, LANES), order[t], jnp.int32) for t in range(sections)]
    own_slot = [[slots[t] == col * rows_dev + l for l in range(rows_dev)] for t in range(sections)]

    for t in range(sections):
        value = jnp.zeros((chips, LANES), jnp.float32)
        for l in range(rows_dev):
            value = jnp.where(own_slot[t][l], rhs[:, l, :], value)
        for j in range(chips):
            b_out[j, t] = value[j : j + 1]

    masks = [
        [
            jnp.where(own_slot[t][l], 1.0, 0.0).astype(jnp.bfloat16)[None]
            for l in range(rows_dev)
        ]
        for t in range(sections)
    ]

    def own_half(t, u, part):
        value = None
        for l in range(rows_dev):
            start = pl.multiple_of(l * tile + part * half, half)
            rows = fac[u, pl.ds(start, half), :].reshape(half // chips, chips, LANES)
            rows = rows * masks[t][l]
            value = rows if value is None else value + rows
        return value.reshape(chips, half // chips, LANES)

    def tiles_of(t):
        return pl.ds(first_of(t), len(moved(t)))

    def share(t):
        for u in moved(t):
            core_out[place_of(t, u)] = own_half(t, u, 1 - core)
        send(("core", t), core_out.at[tiles_of(t)], core_in.at[tiles_of(t)], {"core": 1 - core})

    def keep_own(t):
        for u in moved(t):
            plane_out[place_of(t, u)] = own_half(t, u, core)

    def to_chips(key, source, target):
        for step in steps:
            py, px = chip_at(step)
            for other in range(2):
                send(
                    key,
                    source.at[py * nx + px],
                    target.at[col],
                    {"y": py, "x": px, "core": (core + other) % 2},
                )
        send(key, source.at[chip], target.at[col], {"core": 1 - core})

    def from_chips(key, target):
        arrived(key, target.at[pl.ds(0, 2 * chips - 1)])
        value = target[0]
        for j in range(1, 2 * chips):
            value = value + target[j]
        return value

    with jax.named_scope("barrier"):
        pl.semaphore_wait(barrier, count)
    to_chips(("b",), b_out, b_in)
    b_in[col] = b_out[chip]

    def scatter(t):
        arrived(("core", t), core_in.at[tiles_of(t)])
        for q in range(first_of(t), first_of(t + 1)):
            plane_out[q] = plane_out[q] + core_in[q]
            plane_in[chip, q] = plane_out[q, chip]
        for step in steps:
            py, px = chip_at(step)
            send(
                ("scatter", t),
                plane_out.at[tiles_of(t), py * nx + px],
                plane_in.at[chip, tiles_of(t)],
                {"y": py, "x": px},
            )

    def gather(t):
        arrived(("scatter", t), plane_in.at[pl.ds(0, chips - 1), tiles_of(t)])
        for q in range(first_of(t), first_of(t + 1)):
            value = plane_in[0, q]
            for j in range(1, chips):
                value = value + plane_in[j, q]
            chunk[q] = value
            low[q, core, chip] = value
        for step in steps:
            py, px = chip_at(step)
            send(
                ("gather", t),
                chunk.at[tiles_of(t)],
                low.at[tiles_of(t), core, chip],
                {"y": py, "x": px},
            )

    def swap(t):
        arrived(("gather", t), low.at[tiles_of(t), 0, pl.ds(0, chips - 1)])
        send(
            ("swap", t),
            low.at[tiles_of(t), core],
            low.at[tiles_of(t), core],
            {"core": 1 - core},
        )

    def swapped(t):
        arrived(("swap", t), low.at[tiles_of(t), 0])

    block_row = lax.broadcasted_iota(jnp.int32, (nz, LANES), 0)
    held = [jnp.zeros((nz, LANES), jnp.float32) for _ in range(sections)]
    sent = [None] * sections

    def product(t, u):
        weights = low[place_of(t, u)].reshape(tile, LANES)
        full = lax.dot_general(
            sent[u], weights, (((1,), (1,)), ((), ())), preferred_element_type=jnp.float32
        )
        value = jnp.zeros((nz, LANES), jnp.float32)
        for k in range(nz):
            value = jnp.where(block_row == k, full[0:nz, k * LANES : (k + 1) * LANES], value)
        return value

    def add(t, u):
        held[t] = held[t] + product(t, u)

    def ask(t, b_all):
        value = jnp.where(block_row == z, b_all[t], 0.0) - held[t]
        z_out[t] = value
        z_in[t, z] = value
        for step in z_steps:
            send(("z", t), z_out.at[t], z_in.at[t, z], {"row": z_at(step)})

    def solve(t):
        arrived(("z", t), z_in.at[t, pl.ds(0, nz - 1)])
        remaining = z_in[t, 0]
        for k in range(1, nz):
            remaining = remaining + z_in[t, k]
        high = remaining.astype(jnp.bfloat16).astype(jnp.float32)
        rest = remaining - high
        mid = rest.astype(jnp.bfloat16).astype(jnp.float32)
        pieces = jnp.concatenate([high, mid, rest - mid, jnp.zeros_like(high)], axis=0)
        piece_row = lax.broadcasted_iota(jnp.int32, (4 * nz, LANES), 0) % nz
        spread = jnp.concatenate(
            [jnp.where(piece_row == k, pieces, 0.0) for k in range(nz)], axis=1
        ).astype(jnp.bfloat16)
        parts = lax.dot_general(
            spread, inv[t], (((1,), (1,)), ((), ())), preferred_element_type=jnp.float32
        )
        solved = jnp.sum(parts, axis=0, keepdims=True)
        x_all[t, chip] = solved
        for step in steps:
            py, px = chip_at(step)
            send(("x", t), x_all.at[t, chip], x_all.at[t, chip], {"y": py, "x": px})
        kept = jnp.where(t < my_live, jnp.broadcast_to(solved, (chips, LANES)), 0.0)
        sent[t] = kept.astype(jnp.bfloat16)

    rhs_row = lax.broadcasted_iota(jnp.int32, (chips, LANES), 0)
    live_rows = jnp.zeros((chips, LANES), jnp.int32)
    for j in range(chips):
        live_rows = jnp.where(rhs_row == j, live[j], live_rows)
    my_live = jnp.full((chips, LANES), live[chip], jnp.int32)
    solved_all = [None] * sections

    def update(u):
        arrived(("x", u), x_all.at[u, pl.ds(0, chips - 1)])
        rows = jnp.concatenate([x_all[u, j] for j in range(chips)], axis=0)
        solved_all[u] = rows
        block = jnp.where(u < live_rows, rows, 0.0).astype(jnp.bfloat16)
        for l in range(rows_dev):
            part = lax.dot_general(
                block,
                fac[u, l * tile : (l + 1) * tile, :],
                (((1,), (1,)), ((), ())),
                preferred_element_type=jnp.float32,
            )
            total[l] = part if u == 0 else total[l] + part

    def back(t):
        i = t - NEAR - 1
        for k in range(nz):
            value = jnp.zeros((chips, LANES), jnp.float32)
            for l in range(rows_dev):
                part = total[l, :, k * LANES : (k + 1) * LANES]
                value = jnp.where(own_slot[t][l], part, value)
            back_out[i, :, k, :] = value
        to_chips(("back", t), back_out.at[i], back_in.at[i])
        back_in[i, col] = back_out[i, chip]

    def backed(t):
        i = t - NEAR - 1
        held[t] = held[t] + from_chips(("back", t), back_in.at[i])

    fac_copies[0].wait()
    share(1)
    keep_own(1)
    fac_copies[1].wait()
    share(2)
    scatter(1)
    keep_own(2)
    scatter(2)
    fac_copies[2].wait()
    share(3)
    fac_copies[3].wait()
    share(4)
    keep_own(3)
    keep_own(4)
    b_all = from_chips(("b",), b_in)
    ask(0, b_all)
    gather(1)
    scatter(3)
    gather(2)
    inv_copy.wait()
    solve(0)
    scatter(4)
    swap(1)
    swapped(1)
    add(1, 0)
    ask(1, b_all)
    gather(3)
    swap(2)
    update(0)
    back(3)
    swapped(2)
    add(2, 0)
    solve(1)
    add(2, 1)
    ask(2, b_all)
    gather(4)
    swap(3)
    update(1)
    back(4)
    swapped(3)
    add(3, 1)
    backed(3)
    solve(2)
    add(3, 2)
    ask(3, b_all)
    swap(4)
    swapped(4)
    add(4, 2)
    backed(4)
    update(2)
    solve(3)
    add(4, 3)
    ask(4, b_all)
    update(3)
    fac_copies[4].wait()
    solve(4)
    update(4)

    for k in range(nz):
        f_out[k] = total[:, :, k * LANES : (k + 1) * LANES].astype(jnp.bfloat16)
    for step in z_steps:
        to = z_at(step)
        send(("final",), f_out.at[to], f_in.at[z], {"row": to})
    f_in[z] = f_out[z]
    bases = []
    for l in range(rows_dev):
        base = rhs[:, l, :]
        scale = jnp.ones_like(base)
        for u in range(sections):
            here = (u < live_rows) & own_slot[u][l]
            base = jnp.where(here, solved_all[u], base)
            scale = jnp.where(here, 0.0, scale)
        bases.append((base, scale))

    def left(key, like):
        pltpu.make_async_copy(like, like, send_sem.at[phase(*key)]).wait()

    left(("b",), b_in.at[pl.ds(0, 2 * chips - 1)])
    for t in range(1, sections):
        left(("core", t), core_out.at[tiles_of(t)])
        left(("scatter", t), plane_in.at[pl.ds(0, chips - 1), tiles_of(t)])
        left(("gather", t), plane_in.at[pl.ds(0, chips - 1), tiles_of(t)])
        left(("swap", t), low.at[tiles_of(t), 0])
    for t in range(NEAR + 1, sections):
        left(("back", t), back_in.at[t - NEAR - 1, pl.ds(0, 2 * chips - 1)])
    for t in range(sections):
        left(("z", t), z_in.at[t, pl.ds(0, nz - 1)])
        left(("x", t), x_all.at[t, pl.ds(0, chips - 1)])

    arrived(("final",), f_in.at[pl.ds(0, nz - 1)])
    for l in range(rows_dev):
        taken = f_in[0, l].astype(jnp.float32)
        for k in range(1, nz):
            taken = taken + f_in[k, l].astype(jnp.float32)
        base, scale = bases[l]
        out[:, l, :] = base - jnp.where(scale > 0.5, taken, 0.0)
    left(("final",), f_in.at[pl.ds(0, nz - 1)])


def per_device(sizes, factor, diag_inverse, right_side, tile_order, live_segments):
    nz, ny, nx = sizes
    sections, _, tile = diag_inverse.shape
    rhs_count, rows_dev, width = right_side.shape
    chips = ny * nx
    tiles = first_of(sections)
    part = tile // (2 * chips)
    phases = 2 + 4 * (sections - 1) + 2 * sections + sections - NEAR - 1
    bf16, f32 = jnp.bfloat16, jnp.float32
    vmem = pltpu.VMEM
    return pl.pallas_call(
        functools.partial(kernel, sizes, sections),
        out_shape=jax.ShapeDtypeStruct(right_side.shape, f32),
        in_specs=[
            pl.BlockSpec(memory_space=pltpu.SMEM),
            pl.BlockSpec(memory_space=pltpu.SMEM),
            pl.BlockSpec(memory_space=pl.ANY),
            pl.BlockSpec(memory_space=pl.ANY),
            pl.BlockSpec(memory_space=vmem),
        ],
        out_specs=pl.BlockSpec(memory_space=vmem),
        scratch_shapes=[
            vmem((sections, rows_dev * tile, width), bf16),
            vmem((sections, width, tile), bf16),
            vmem((tiles, 2, chips, part, width), bf16),
            vmem((tiles, chips, part, width), bf16),
            vmem((tiles, chips, part, width), bf16),
            vmem((tiles, chips, part, width), bf16),
            vmem((chips, tiles, part, width), bf16),
            vmem((tiles, part, width), bf16),
            vmem((rhs_count, sections, 1, width), f32),
            vmem((2 * chips, sections, 1, width), f32),
            vmem((sections, nz, width), f32),
            vmem((sections, nz, nz, width), f32),
            vmem((sections, chips, 1, width), f32),
            vmem((rows_dev, rhs_count, tile), f32),
            vmem((sections - NEAR - 1, chips, nz, width), f32),
            vmem((sections - NEAR - 1, 2 * chips, nz, width), f32),
            vmem((nz, rows_dev, rhs_count, width), bf16),
            vmem((nz, rows_dev, rhs_count, width), bf16),
            pltpu.SemaphoreType.DMA((sections + 1,)),
            pltpu.SemaphoreType.DMA((phases,)),
            pltpu.SemaphoreType.DMA((phases,)),
        ],
        compiler_params=pltpu.CompilerParams(collective_id=0, has_side_effects=True),
    )(tile_order, live_segments, jnp.transpose(factor, (1, 0, 2)), diag_inverse, right_side)


def solution(mesh):
    sizes = (mesh.shape["row"], 4, 4)
    finer = Mesh(mesh.devices.reshape(mesh.shape["row"], 4, 4, 2), ("row", *COL))
    return jax.shard_map(
        functools.partial(per_device, sizes),
        mesh=finer,
        in_specs=(P(COL, None, "row"), P(None, "row", None), P(None, COL, "row"), P(), P()),
        out_specs=P(None, COL, "row"),
        check_vma=False,
    )
```

```python
import functools
import itertools

import jax
import jax.numpy as jnp
from jax import lax
from jax.experimental import pallas as pl
from jax.experimental.pallas import tpu as pltpu
from jax.sharding import Mesh
from jax.sharding import PartitionSpec as P

MESH = pl.DeviceIdType.MESH
COL = ("y", "x", "core")
LANES = 128


NEAR = 2


def moved(t):
    return range(max(0, t - NEAR), t)


def first_of(t):
    return sum(len(moved(s)) for s in range(1, t))


def place_of(t, u):
    return first_of(t) + u - moved(t)[0]


def kernel(
    sizes,
    sections,
    order_hbm,
    live_hbm,
    f_hbm,
    d_hbm,
    rhs_hbm,
    out,
    order,
    live,
    rhs,
    fac,
    inv,
    low,
    core_out,
    core_in,
    plane_out,
    plane_in,
    chunk,
    b_out,
    b_in,
    z_out,
    z_in,
    x_all,
    total,
    back_out,
    back_in,
    f_out,
    f_in,
    local_sem,
    send_sem,
    recv_sem,
):
    nz, ny, nx = sizes
    chips = ny * nx
    tile = nz * LANES
    half = tile // 2
    rows_dev = rhs.shape[1]
    z = lax.axis_index("row")
    y = lax.axis_index("y")
    x = lax.axis_index("x")
    core = lax.axis_index("core")
    chip = y * nx + x
    col = chip * 2 + core

    phase_of = {}

    def phase(*key):
        return phase_of.setdefault(key, len(phase_of))

    pending = []

    def send(key, src, dst, device):
        number = phase(*key)
        pltpu.make_async_remote_copy(
            src_ref=src,
            dst_ref=dst,
            send_sem=send_sem.at[number],
            recv_sem=recv_sem.at[number],
            device_id=device,
            device_id_type=MESH,
        ).start()

    def arrived(key, like):
        pltpu.make_async_copy(like, like, recv_sem.at[phase(*key)]).wait()

    steps = sorted(
        [o for o in itertools.product(range(ny), range(nx)) if any(o)],
        key=lambda o: -(min(o[0], ny - o[0]) + min(o[1], nx - o[1])),
    )

    def chip_at(step):
        return lax.rem(y + step[0], ny), lax.rem(x + step[1], nx)

    def z_at(step):
        return lax.rem(z + step, nz)

    z_steps = sorted(range(1, nz), key=lambda o: -min(o, nz - o))

    barrier = pltpu.get_barrier_semaphore()
    count = 0
    for step in steps:
        py, px = chip_at(step)
        for other in range(2):
            pl.semaphore_signal(
                barrier,
                inc=1,
                device_id={"y": py, "x": px, "core": (core + other) % 2},
                device_id_type=MESH,
            )
            count += 1
    for step in z_steps:
        pl.semaphore_signal(barrier, inc=1, device_id={"row": z_at(step)}, device_id_type=MESH)
        count += 1
    pl.semaphore_signal(barrier, inc=1, device_id={"core": 1 - core}, device_id_type=MESH)
    count += 1

    small_copies = []
    for i, (src, dst) in enumerate([(order_hbm, order), (rhs_hbm, rhs), (live_hbm, live)]):
        copy = pltpu.make_async_copy(src, dst, local_sem.at[sections + 1 + i])
        copy.start()
        small_copies.append(copy)
    fac_copies = []
    for u in range(sections):
        copy = pltpu.make_async_copy(f_hbm.at[u], fac.at[u], local_sem.at[u])
        copy.start()
        fac_copies.append(copy)
    inv_copy = pltpu.make_async_copy(d_hbm, inv, local_sem.at[sections])
    inv_copy.start()
    for copy in small_copies:
        copy.wait()

    slots = [jnp.full((chips, LANES), order[t], jnp.int32) for t in range(sections)]
    own_slot = [[slots[t] == col * rows_dev + l for l in range(rows_dev)] for t in range(sections)]

    for t in range(sections):
        value = jnp.zeros((chips, LANES), jnp.float32)
        for l in range(rows_dev):
            value = jnp.where(own_slot[t][l], rhs[:, l, :], value)
        for j in range(chips):
            b_out[j, t] = value[j : j + 1]

    masks = [
        [
            jnp.where(own_slot[t][l], 1.0, 0.0).astype(jnp.bfloat16)[None]
            for l in range(rows_dev)
        ]
        for t in range(sections)
    ]

    def own_half(t, u, part):
        value = None
        for l in range(rows_dev):
            start = pl.multiple_of(l * tile + part * half, half)
            rows = fac[u, pl.ds(start, half), :].reshape(half // chips, chips, LANES)
            rows = rows * masks[t][l]
            value = rows if value is None else value + rows
        return value.reshape(chips, half // chips, LANES)

    def tiles_of(t):
        return pl.ds(first_of(t), len(moved(t)))

    def share(t):
        for u in moved(t):
            core_out[place_of(t, u)] = own_half(t, u, 1 - core)
        send(("core", t), core_out.at[tiles_of(t)], core_in.at[tiles_of(t)], {"core": 1 - core})

    def keep_own(t):
        for u in moved(t):
            plane_out[place_of(t, u)] = own_half(t, u, core)

    def to_chips(key, source, target):
        for step in steps:
            py, px = chip_at(step)
            for other in range(2):
                send(
                    key,
                    source.at[py * nx + px],
                    target.at[col],
                    {"y": py, "x": px, "core": (core + other) % 2},
                )
        send(key, source.at[chip], target.at[col], {"core": 1 - core})

    def from_chips(key, target):
        arrived(key, target.at[pl.ds(0, 2 * chips - 1)])
        value = target[0].astype(jnp.float32)
        for j in range(1, 2 * chips):
            value = value + target[j].astype(jnp.float32)
        return value

    with jax.named_scope("barrier"):
        pl.semaphore_wait(barrier, count)
    to_chips(("b",), b_out, b_in)
    b_in[col] = b_out[chip]

    def scatter(t):
        arrived(("core", t), core_in.at[tiles_of(t)])
        for q in range(first_of(t), first_of(t + 1)):
            plane_out[q] = plane_out[q] + core_in[q]
            plane_in[chip, q] = plane_out[q, chip]
        for step in steps:
            py, px = chip_at(step)
            send(
                ("scatter", t),
                plane_out.at[tiles_of(t), py * nx + px],
                plane_in.at[chip, tiles_of(t)],
                {"y": py, "x": px},
            )

    def gather(t):
        arrived(("scatter", t), plane_in.at[pl.ds(0, chips - 1), tiles_of(t)])
        for q in range(first_of(t), first_of(t + 1)):
            value = plane_in[0, q]
            for j in range(1, chips):
                value = value + plane_in[j, q]
            chunk[q] = value
            low[q, core, chip] = value
        for step in steps:
            py, px = chip_at(step)
            send(
                ("gather", t),
                chunk.at[tiles_of(t)],
                low.at[tiles_of(t), core, chip],
                {"y": py, "x": px},
            )

    def swap(t):
        arrived(("gather", t), low.at[tiles_of(t), 0, pl.ds(0, chips - 1)])
        send(
            ("swap", t),
            low.at[tiles_of(t), core],
            low.at[tiles_of(t), core],
            {"core": 1 - core},
        )

    def swapped(t):
        arrived(("swap", t), low.at[tiles_of(t), 0])

    block_row = lax.broadcasted_iota(jnp.int32, (nz, LANES), 0)
    held = [jnp.zeros((nz, LANES), jnp.float32) for _ in range(sections)]
    sent = [None] * sections

    def product(t, u):
        weights = low[place_of(t, u)].reshape(tile, LANES)
        full = lax.dot_general(
            sent[u], weights, (((1,), (1,)), ((), ())), preferred_element_type=jnp.float32
        )
        value = jnp.zeros((nz, LANES), jnp.float32)
        for k in range(nz):
            value = jnp.where(block_row == k, full[0:nz, k * LANES : (k + 1) * LANES], value)
        return value

    def add(t, u):
        held[t] = held[t] + product(t, u)

    def ask(t, b_all):
        value = jnp.where(block_row == z, b_all[t], 0.0) - held[t]
        z_out[t] = value
        z_in[t, z] = value
        for step in z_steps:
            send(("z", t), z_out.at[t], z_in.at[t, z], {"row": z_at(step)})

    def solve(t):
        arrived(("z", t), z_in.at[t, pl.ds(0, nz - 1)])
        remaining = z_in[t, 0]
        for k in range(1, nz):
            remaining = remaining + z_in[t, k]
        high = remaining.astype(jnp.bfloat16).astype(jnp.float32)
        rest = remaining - high
        mid = rest.astype(jnp.bfloat16).astype(jnp.float32)
        pieces = jnp.concatenate([high, mid, rest - mid, jnp.zeros_like(high)], axis=0)
        piece_row = lax.broadcasted_iota(jnp.int32, (4 * nz, LANES), 0) % nz
        spread = jnp.concatenate(
            [jnp.where(piece_row == k, pieces, 0.0) for k in range(nz)], axis=1
        ).astype(jnp.bfloat16)
        parts = lax.dot_general(
            spread, inv[t], (((1,), (1,)), ((), ())), preferred_element_type=jnp.float32
        )
        solved = jnp.sum(parts, axis=0, keepdims=True)
        x_all[t, chip] = solved
        for step in steps:
            py, px = chip_at(step)
            send(("x", t), x_all.at[t, chip], x_all.at[t, chip], {"y": py, "x": px})
        kept = jnp.where(t < my_live, jnp.broadcast_to(solved, (chips, LANES)), 0.0)
        sent[t] = kept.astype(jnp.bfloat16)

    rhs_row = lax.broadcasted_iota(jnp.int32, (chips, LANES), 0)
    live_rows = jnp.zeros((chips, LANES), jnp.int32)
    for j in range(chips):
        live_rows = jnp.where(rhs_row == j, live[j], live_rows)
    my_live = jnp.full((chips, LANES), live[chip], jnp.int32)
    solved_all = [None] * sections

    def update(u):
        arrived(("x", u), x_all.at[u, pl.ds(0, chips - 1)])
        rows = jnp.concatenate([x_all[u, j] for j in range(chips)], axis=0)
        solved_all[u] = rows
        block = jnp.where(u < live_rows, rows, 0.0).astype(jnp.bfloat16)
        for l in range(rows_dev):
            part = lax.dot_general(
                block,
                fac[u, l * tile : (l + 1) * tile, :],
                (((1,), (1,)), ((), ())),
                preferred_element_type=jnp.float32,
            )
            total[l] = part if u == 0 else total[l] + part

    def back(t):
        i = t - NEAR - 1
        for k in range(nz):
            value = jnp.zeros((chips, LANES), jnp.float32)
            for l in range(rows_dev):
                part = total[l, :, k * LANES : (k + 1) * LANES]
                value = jnp.where(own_slot[t][l], part, value)
            back_out[i, :, k, :] = value.astype(back_out.dtype)
        to_chips(("back", t), back_out.at[i], back_in.at[i])
        back_in[i, col] = back_out[i, chip]

    def backed(t):
        i = t - NEAR - 1
        held[t] = held[t] + from_chips(("back", t), back_in.at[i])

    fac_copies[0].wait()
    share(1)
    keep_own(1)
    fac_copies[1].wait()
    share(2)
    scatter(1)
    keep_own(2)
    scatter(2)
    fac_copies[2].wait()
    share(3)
    fac_copies[3].wait()
    share(4)
    keep_own(3)
    keep_own(4)
    b_all = from_chips(("b",), b_in)
    ask(0, b_all)
    gather(1)
    scatter(3)
    inv_copy.wait()
    solve(0)
    gather(2)
    scatter(4)
    swap(1)
    swapped(1)
    add(1, 0)
    ask(1, b_all)
    gather(3)
    update(0)
    back(3)
    swap(2)
    swapped(2)
    add(2, 0)
    solve(1)
    add(2, 1)
    ask(2, b_all)
    gather(4)
    swap(3)
    swapped(3)
    add(3, 1)
    backed(3)
    solve(2)
    add(3, 2)
    ask(3, b_all)
    update(1)
    back(4)
    swap(4)
    swapped(4)
    add(4, 2)
    backed(4)
    solve(3)
    add(4, 3)
    ask(4, b_all)
    update(2)
    fac_copies[4].wait()
    solve(4)
    update(3)
    update(4)

    for k in range(nz):
        f_out[k] = total[:, :, k * LANES : (k + 1) * LANES].astype(jnp.bfloat16)
    for step in z_steps:
        to = z_at(step)
        send(("final",), f_out.at[to], f_in.at[z], {"row": to})
    f_in[z] = f_out[z]
    bases = []
    for l in range(rows_dev):
        base = rhs[:, l, :]
        scale = jnp.ones_like(base)
        for u in range(sections):
            here = (u < live_rows) & own_slot[u][l]
            base = jnp.where(here, solved_all[u], base)
            scale = jnp.where(here, 0.0, scale)
        bases.append((base, scale))

    def left(key, like):
        pltpu.make_async_copy(like, like, send_sem.at[phase(*key)]).wait()

    left(("b",), b_in.at[pl.ds(0, 2 * chips - 1)])
    for t in range(1, sections):
        left(("core", t), core_out.at[tiles_of(t)])
        left(("scatter", t), plane_in.at[pl.ds(0, chips - 1), tiles_of(t)])
        left(("gather", t), plane_in.at[pl.ds(0, chips - 1), tiles_of(t)])
        left(("swap", t), low.at[tiles_of(t), 0])
    for t in range(NEAR + 1, sections):
        left(("back", t), back_in.at[t - NEAR - 1, pl.ds(0, 2 * chips - 1)])
    for t in range(sections):
        left(("z", t), z_in.at[t, pl.ds(0, nz - 1)])
        left(("x", t), x_all.at[t, pl.ds(0, chips - 1)])

    arrived(("final",), f_in.at[pl.ds(0, nz - 1)])
    for l in range(rows_dev):
        taken = f_in[0, l].astype(jnp.float32)
        for k in range(1, nz):
            taken = taken + f_in[k, l].astype(jnp.float32)
        base, scale = bases[l]
        out[:, l, :] = base - jnp.where(scale > 0.5, taken, 0.0)
    left(("final",), f_in.at[pl.ds(0, nz - 1)])


def per_device(sizes, factor, diag_inverse, right_side, tile_order, live_segments):
    nz, ny, nx = sizes
    sections, _, tile = diag_inverse.shape
    rhs_count, rows_dev, width = right_side.shape
    chips = ny * nx
    tiles = first_of(sections)
    part = tile // (2 * chips)
    phases = 2 + 4 * (sections - 1) + 2 * sections + sections - NEAR - 1
    bf16, f32 = jnp.bfloat16, jnp.float32
    vmem = pltpu.VMEM
    return pl.pallas_call(
        functools.partial(kernel, sizes, sections),
        out_shape=vmem(right_side.shape, f32),
        in_specs=[
            pl.BlockSpec(memory_space=pl.ANY),
            pl.BlockSpec(memory_space=pl.ANY),
            pl.BlockSpec(memory_space=pl.ANY),
            pl.BlockSpec(memory_space=pl.ANY),
            pl.BlockSpec(memory_space=pl.ANY),
        ],
        out_specs=pl.BlockSpec(memory_space=vmem),
        scratch_shapes=[
            pltpu.SMEM(tile_order.shape, jnp.int32),
            pltpu.SMEM(live_segments.shape, jnp.int32),
            vmem(right_side.shape, f32),
            vmem((sections, rows_dev * tile, width), bf16),
            vmem((sections, width, tile), bf16),
            vmem((tiles, 2, chips, part, width), bf16),
            vmem((tiles, chips, part, width), bf16),
            vmem((tiles, chips, part, width), bf16),
            vmem((tiles, chips, part, width), bf16),
            vmem((chips, tiles, part, width), bf16),
            vmem((tiles, part, width), bf16),
            vmem((rhs_count, sections, 1, width), f32),
            vmem((2 * chips, sections, 1, width), f32),
            vmem((sections, nz, width), f32),
            vmem((sections, nz, nz, width), f32),
            vmem((sections, chips, 1, width), f32),
            vmem((rows_dev, rhs_count, tile), f32),
            vmem((sections - NEAR - 1, chips, nz, width), bf16),
            vmem((sections - NEAR - 1, 2 * chips, nz, width), bf16),
            vmem((nz, rows_dev, rhs_count, width), bf16),
            vmem((nz, rows_dev, rhs_count, width), bf16),
            pltpu.SemaphoreType.DMA((sections + 4,)),
            pltpu.SemaphoreType.DMA((phases,)),
            pltpu.SemaphoreType.DMA((phases,)),
        ],
        compiler_params=pltpu.CompilerParams(collective_id=0, has_side_effects=True),
    )(tile_order, live_segments, jnp.transpose(factor, (1, 0, 2)), diag_inverse, right_side)


def solution(mesh):
    sizes = (mesh.shape["row"], 4, 4)
    finer = Mesh(mesh.devices.reshape(mesh.shape["row"], 4, 4, 2), ("row", *COL))
    return jax.shard_map(
        functools.partial(per_device, sizes),
        mesh=finer,
        in_specs=(P(COL, None, "row"), P(None, "row", None), P(None, COL, "row"), P(), P()),
        out_specs=P(None, COL, "row"),
        check_vma=False,
    )
```
